32 devices in a mesh: tm: 2 (over x), py: 4 (over y, core), pz: 4 (over z).
Axes of the slice: x: 2, y: 2, z: 4, core: 2. Of those that a mesh axis runs over, the one named last changes fastest.
Arguments:
- start_states: float32 [2, 3, 128, 8, 16, 128], P('tm', None, None, None, ('py', 'pz')), may hold values from -6 to 6
Outputs:
- new_states: float32 [2, 3, 128, 8, 16, 128], P('tm', None, None, None, ('py', 'pz'))
The draws below stay inside these ranges and needn't reach their ends.
All inputs are finite; a program needn't handle non-finite values.
Results may differ from the reference program's by a relative error of at most 0.0001.
Values sent between devices are 32-bit elements; how exact they have to be, the bound alone decides.
A program may use at most 128 MiB of HBM per device.

```python
import jax
import jax.numpy as jnp
from jax import lax

N = 128
M = 64
PEN = 16
SLICES = 2


def shard_levels(rng, shape, shards, least, high):
    level = 1.0
    for dim, shards_of in shards:
        draws = jax.random.uniform(jax.random.fold_in(jax.random.fold_in(rng, 6), dim), (shards_of,), jnp.float32, least / len(shards), high / len(shards))
        level = level * jnp.repeat(jnp.exp(draws), shape[dim] // shards_of).reshape((-1,) + (1,) * (len(shape) - 1 - dim))
    return level


def bell_draw(rng, shape, width, most, cuts=(), kind=jnp.bfloat16):
    entries = width * jax.random.normal(rng, shape, jnp.float32)
    if cuts:
        entries = entries * shard_levels(rng, shape, cuts, -0.22, 0.18)
    return jnp.clip(entries, -most, most).astype(kind)


def setup_inputs(seed: int = 0) -> dict:
    arg_keys = jax.random.split(jax.random.key(seed), 2)
    return {
        "start_states": bell_draw(arg_keys[0], (SLICES, 3, N, N // PEN, PEN, N), 1.0, 6.0, ((0, 2), (4, 16)), jnp.float32),
    }


viscosity = 0.03
time_step = 0.004


def signed_wave(length):
    places = jnp.arange(length, dtype=jnp.int32)
    return jnp.where(places < length // 2, places, places - length).astype(jnp.float32)


def wavenumbers(retained):
    wave_x = signed_wave(retained)[:, None, None]
    wave_y = signed_wave(retained)[None, :, None]
    wave_z = jnp.arange(retained // 2, dtype=jnp.int32).astype(jnp.float32)[None, None, :]
    return wave_x, wave_y, wave_z


def vorticity(coeffs, wavegrid):
    wave_x, wave_y, wave_z = wavegrid
    along_x = 1j * (wave_y * coeffs[2] - wave_z * coeffs[1])
    along_y = 1j * (wave_z * coeffs[0] - wave_x * coeffs[2])
    along_z = 1j * (wave_x * coeffs[1] - wave_y * coeffs[0])
    return jnp.stack([along_x, along_y, along_z])


def project(coeffs, wavegrid):
    wave_x, wave_y, wave_z = wavegrid
    squared = wave_x * wave_x + wave_y * wave_y + wave_z * wave_z
    divergence = (wave_x * coeffs[0] + wave_y * coeffs[1] + wave_z * coeffs[2]) / jnp.maximum(squared, 1.0)
    return jnp.stack([coeffs[0] - wave_x * divergence, coeffs[1] - wave_y * divergence, coeffs[2] - wave_z * divergence])


def cross_product(first_field, second_field):
    return jnp.stack([
        first_field[1] * second_field[2] - first_field[2] * second_field[1],
        first_field[2] * second_field[0] - first_field[0] * second_field[2],
        first_field[0] * second_field[1] - first_field[1] * second_field[0],
    ])


def widen(coeffs, extent, contracted):
    length = coeffs.shape[contracted]
    halfway = length // 2
    low_part = lax.slice_in_dim(coeffs, 0, halfway, axis=contracted)
    high_part = lax.slice_in_dim(coeffs, halfway, length, axis=contracted)
    filler_shape = list(coeffs.shape)
    filler_shape[contracted] = extent - length
    return jnp.concatenate([low_part, jnp.zeros(filler_shape, coeffs.dtype), high_part], axis=contracted)


def narrow(coeffs, kept, contracted):
    length = coeffs.shape[contracted]
    halfway = kept // 2
    low_part = lax.slice_in_dim(coeffs, 0, halfway, axis=contracted)
    high_part = lax.slice_in_dim(coeffs, length - halfway, length, axis=contracted)
    return jnp.concatenate([low_part, high_part], axis=contracted)


def widen_last(coeffs, columns):
    filler_shape = list(coeffs.shape)
    filler_shape[3] = columns - coeffs.shape[3]
    return jnp.concatenate([coeffs, jnp.zeros(filler_shape, coeffs.dtype)], axis=3)


def to_physical(coeffs, extent):
    retained = coeffs.shape[1]
    spread = widen(widen(coeffs, extent, 1), extent, 2)
    spread = widen_last(spread, extent // 2 + 1)
    spread = jnp.fft.ifft(spread, axis=1)
    spread = jnp.fft.ifft(spread, axis=2)
    constant_column = jnp.real(spread[..., :1]).astype(spread.dtype)
    spread = jnp.concatenate([constant_column, spread[..., 1:]], axis=3)
    return jnp.fft.irfft(spread, n=extent, axis=3) * (extent ** 3 / retained ** 1.5)


def to_spectral(fields, retained):
    extent = fields.shape[-1]
    spectrum = jnp.fft.rfftn(fields, axes=(1, 2, 3))
    spectrum = narrow(narrow(spectrum, retained, 1), retained, 2)[..., : retained // 2]
    return spectrum * (retained ** 1.5 / extent ** 3)


def restrict(coeffs, kept):
    return narrow(narrow(coeffs, kept, 1), kept, 2)[..., : kept // 2]


def prolong(coeffs, retained):
    wider = widen(widen(coeffs, retained, 1), retained, 2)
    return widen_last(wider, retained // 2)


def advance(coeffs):
    retained = coeffs.shape[1]
    extent = 3 * retained // 2
    wavegrid = wavenumbers(retained)
    fields = to_physical(jnp.concatenate([coeffs, vorticity(coeffs, wavegrid)], axis=0), extent)
    product = cross_product(fields[:3], fields[3:])
    nonlinear = to_spectral(product, retained)
    wave_x, wave_y, wave_z = wavegrid
    squared = wave_x * wave_x + wave_y * wave_y + wave_z * wave_z
    damping = jnp.exp(-viscosity * time_step * squared)
    return damping * (coeffs + time_step * project(nonlinear, wavegrid))


def pack(coeffs):
    merged = jnp.concatenate([jnp.real(coeffs), jnp.imag(coeffs)], axis=-1).astype(jnp.float32)
    return merged.reshape(3, N, N // PEN, PEN, N)


def unpack(stored):
    merged = stored.reshape(3, N, N, N)
    return merged[..., : N // 2] + 1j * merged[..., N // 2:]


def reference(start_states):
    slices = start_states.shape[0]
    fine_ends = []
    corrections = []
    first_state = None
    for slice_number in range(slices):
        spectral_state = project(unpack(start_states[slice_number]), wavenumbers(N))
        if slice_number == 0:
            first_state = spectral_state
        fine_end = advance(spectral_state)
        coarse_next = advance(restrict(spectral_state, M))
        fine_ends.append(fine_end)
        corrections.append(restrict(fine_end, M) - coarse_next)
    chained = restrict(fine_ends[0], M)
    packed = [pack(first_state)]
    for slice_number in range(1, slices):
        previous = fine_ends[slice_number - 1]
        upper_band = previous - prolong(restrict(previous, M), N)
        packed.append(pack(prolong(chained, N) + upper_band))
        if slice_number < slices - 1:
            chained = advance(chained) + corrections[slice_number]
    return jnp.stack(packed)
```

```python
from functools import partial
import math

import jax
import jax.numpy as jnp
from jax import lax
import numpy as np
from jax.experimental import pallas as pl
from jax.experimental.pallas import tpu as pltpu
from jax.sharding import PartitionSpec as P

M = 64


viscosity = 0.03
time_step = 0.004
highest = lax.Precision.HIGHEST


def shifted(block, axis, distance):
    devices = range(lax.axis_size(axis))
    route = [(i - distance, i) for i in devices if i - distance in devices]
    return lax.ppermute(block, axis, route)


def signed_wave(places, length):
    return jnp.where(places < length // 2, places, places - length)


def rotate(values):
    halfway = values.shape[-1] // 2
    return jnp.concatenate([-values[..., halfway:], values[..., :halfway]], axis=-1)


def trig_pair(outer, inner, extent, factor):
    residue = jnp.mod(outer[:, None] * inner[None, :], extent)
    radians = residue.astype(jnp.float32) * (2.0 * math.pi / extent)
    return (jnp.cos(radians) * factor, jnp.sin(radians) * factor)


def complex_apply(cosine_part, sine_part, values, contracted, direction_sign):
    kernel = jnp.stack(
        [
            jnp.stack([cosine_part, -direction_sign * sine_part]),
            jnp.stack([direction_sign * sine_part, cosine_part]),
        ]
    )
    halfway = values.shape[-1] // 2
    split = values.reshape(values.shape[:-1] + (2, halfway))
    if contracted == 1:
        pattern = "pqok,fkaqh->foaph"
    else:
        pattern = "pqok,flkqh->floph"
    result = jnp.einsum(pattern, kernel, split, precision=highest)
    return result.reshape(result.shape[:-2] + (2 * halfway,))


def inverse_z(extent, retained):
    halfway = retained // 2
    columns = jnp.arange(retained, dtype=jnp.int32)
    harmonic = columns % halfway
    weight = jnp.where(harmonic == 0, 1.0, 2.0) * retained ** (-0.5)
    residue = jnp.mod(harmonic[:, None] * jnp.arange(extent, dtype=jnp.int32)[None, :], extent)
    radians = residue.astype(jnp.float32) * (2.0 * math.pi / extent)
    return (
        jnp.where((columns < halfway)[:, None], jnp.cos(radians), -jnp.sin(radians))
        * weight[:, None]
    )


def forward_z(extent, retained):
    halfway = retained // 2
    columns = jnp.arange(retained, dtype=jnp.int32)
    harmonic = columns % halfway
    residue = jnp.mod(jnp.arange(extent, dtype=jnp.int32)[:, None] * harmonic[None, :], extent)
    radians = residue.astype(jnp.float32) * (2.0 * math.pi / extent)
    return jnp.where((columns < halfway)[None, :], jnp.cos(radians), -jnp.sin(radians)) * (
        math.sqrt(retained) / extent
    )


def inverse_tail(portion, extent, sectioned, layout):
    count_py, count_pz, groups, member = layout
    retained = portion.shape[2]
    local_rows = retained // groups
    places = jnp.arange(retained, dtype=jnp.int32)
    owners = places // local_rows
    wave_y = signed_wave(places % local_rows * groups + owners, retained)
    points = jnp.arange(extent, dtype=jnp.int32)
    cosine_part, sine_part = trig_pair(points, wave_y, extent, retained ** (-0.5))
    along_y = complex_apply(cosine_part, sine_part, portion, 2, 1.0)
    return jnp.einsum("flyr,rz->flyz", along_y, inverse_z(extent, retained), precision=highest)


def forward_tail(portion, retained, sectioned, layout):
    count_py, count_pz, groups, member = layout
    extent = portion.shape[1]
    local_rows = extent // groups
    places = jnp.arange(extent, dtype=jnp.int32)
    points = places // local_rows * local_rows + places % local_rows
    wave_x = signed_wave(jnp.arange(retained, dtype=jnp.int32), retained)
    cosine_part, sine_part = trig_pair(wave_x, points, extent, math.sqrt(retained) / extent)
    return complex_apply(cosine_part, sine_part, portion, 1, -1.0)


def to_physical(coeffs, wavegrid, extent, resolution, layout):
    wave_x, wave_y, wave_z = wavegrid
    retained = coeffs.shape[1]
    seeds = jnp.concatenate([coeffs, wave_x * coeffs[1:3]], axis=0)
    points = jnp.arange(extent, dtype=jnp.int32)
    wave_rows = signed_wave(jnp.arange(retained, dtype=jnp.int32), retained)
    cosine_part, sine_part = trig_pair(points, wave_rows, extent, retained ** (-0.5))
    moved_x = complex_apply(cosine_part, sine_part, seeds, 1, 1.0)
    curl_x = rotate(wave_y * moved_x[2] - wave_z * moved_x[1])
    curl_y = rotate(wave_z * moved_x[0] - moved_x[4])
    curl_z = rotate(moved_x[3] - wave_y * moved_x[0])
    spread = jnp.concatenate([moved_x[:3], jnp.stack([curl_x, curl_y, curl_z])], axis=0)
    if resolution == "coarse":
        finish = partial(inverse_tail, extent=extent, sectioned=False, layout=layout)
        return finish(lax.all_to_all(spread, ("py", "pz"), split_axis=1, concat_axis=2, tiled=True))
    else:
        finish = partial(inverse_tail, extent=extent, sectioned=False, layout=layout)
        return finish(lax.all_to_all(spread, ("py", "pz"), split_axis=1, concat_axis=2, tiled=True))


def to_spectral(fields, retained, resolution, layout):
    count_py, count_pz, groups, member = layout
    extent = fields.shape[-1]
    along_z = jnp.einsum("flyz,zr->flyr", fields, forward_z(extent, retained), precision=highest)
    local_rows = retained // groups
    places = jnp.arange(retained, dtype=jnp.int32)
    wave_y = signed_wave(places % local_rows * groups + places // local_rows, retained)
    cosine_part, sine_part = trig_pair(
        wave_y, jnp.arange(extent, dtype=jnp.int32), extent, math.sqrt(retained) / extent
    )
    along_y = complex_apply(cosine_part, sine_part, along_z, 2, -1.0)
    if resolution == "coarse":
        finish = partial(forward_tail, retained=retained, sectioned=False, layout=layout)
        return finish(
            lax.all_to_all(along_y, ("py", "pz"), split_axis=2, concat_axis=1, tiled=True)
        )
    else:
        finish = partial(forward_tail, retained=retained, sectioned=False, layout=layout)
        return finish(
            lax.all_to_all(along_y, ("py", "pz"), split_axis=2, concat_axis=1, tiled=True)
        )


def wave_grid(retained, layout):
    count_py, count_pz, groups, member = layout
    places = jnp.arange(retained, dtype=jnp.int32)
    wave_x = signed_wave(places, retained).astype(jnp.float32)[:, None, None]
    local_places = jnp.arange(retained // groups, dtype=jnp.int32)
    wave_y = signed_wave(local_places * groups + member, retained).astype(jnp.float32)[
        None, :, None
    ]
    wave_z = (places % (retained // 2)).astype(jnp.float32)[None, None, :]
    return (wave_x, wave_y, wave_z)


def project(coeffs, wavegrid):
    wave_x, wave_y, wave_z = wavegrid
    squared = wave_x * wave_x + wave_y * wave_y + wave_z * wave_z
    divergence = (wave_x * coeffs[0] + wave_y * coeffs[1] + wave_z * coeffs[2]) / jnp.maximum(
        squared, 1.0
    )
    return jnp.stack(
        [
            coeffs[0] - wave_x * divergence,
            coeffs[1] - wave_y * divergence,
            coeffs[2] - wave_z * divergence,
        ]
    )


def cross_product(first_field, second_field):
    return jnp.stack(
        [
            first_field[1] * second_field[2] - first_field[2] * second_field[1],
            first_field[2] * second_field[0] - first_field[0] * second_field[2],
            first_field[0] * second_field[1] - first_field[1] * second_field[0],
        ]
    )


def advance(coeffs, resolution, layout):
    retained = coeffs.shape[1]
    extent = 3 * retained // 2
    wavegrid = wave_grid(retained, layout)
    fields = to_physical(coeffs, wavegrid, extent, resolution, layout)
    product = cross_product(fields[:3], fields[3:])
    nonlinear = to_spectral(product, retained, resolution, layout)
    wave_x, wave_y, wave_z = wavegrid
    squared = wave_x * wave_x + wave_y * wave_y + wave_z * wave_z
    damping = jnp.exp(-viscosity * time_step * squared)
    return damping * (coeffs + time_step * project(nonlinear, wavegrid))


def restrict(coeffs, kept, groups):
    halfway = kept // 2
    retained = coeffs.shape[1]
    rows_kept = jnp.concatenate([coeffs[:, :halfway], coeffs[:, retained - halfway :]], axis=1)
    local_rows = coeffs.shape[2]
    local_kept = kept // groups // 2
    rows_kept = jnp.concatenate(
        [rows_kept[:, :, :local_kept], rows_kept[:, :, local_rows - local_kept :]], axis=2
    )
    columns_half = coeffs.shape[3] // 2
    return jnp.concatenate(
        [rows_kept[..., :halfway], rows_kept[..., columns_half : columns_half + halfway]], axis=3
    )


def prolong(coeffs, retained, groups):
    components, kept, local_kept, width = coeffs.shape
    halfway = kept // 2
    zeros_x = jnp.zeros((components, retained - kept, local_kept, width), jnp.float32)
    wider = jnp.concatenate([coeffs[:, :halfway], zeros_x, coeffs[:, halfway:]], axis=1)
    local_rows = retained // groups
    split_rows = local_kept // 2
    zeros_y = jnp.zeros((components, retained, local_rows - local_kept, width), jnp.float32)
    wider = jnp.concatenate([wider[:, :, :split_rows], zeros_y, wider[:, :, split_rows:]], axis=2)
    zeros_z = jnp.zeros((components, retained, local_rows, retained // 2 - halfway), jnp.float32)
    return jnp.concatenate([wider[..., :halfway], zeros_z, wider[..., halfway:], zeros_z], axis=3)


def wave_table(length):
    places = np.arange(length)
    return np.where(places < length // 2, places, places - length)


def trig_table(outer, inner, extent):
    radians = 2.0 * np.pi / extent * np.mod(np.outer(outer, inner), extent)
    return np.cos(radians), np.sin(radians)


def split_table(table):
    table = np.asarray(table, np.float32)
    high = table.astype(jnp.bfloat16)
    low = (table - high.astype(np.float32)).astype(jnp.bfloat16)
    return high, low


def split(values):
    high = values.astype(jnp.bfloat16)
    low = (values - high.astype(jnp.float32)).astype(jnp.bfloat16)
    return high, low


def dot3(left, right):
    def dot(a, b):
        return jnp.dot(a, b, preferred_element_type=jnp.float32)

    return dot(left[0], right[0]) + dot(left[0], right[1]) + dot(left[1], right[0])


def z_tables(extent, retained):
    halfway = retained // 2
    columns = np.arange(retained)
    harmonic = columns % halfway
    cosine, sine = trig_table(harmonic, np.arange(extent), extent)
    table = np.where((columns < halfway)[:, None], cosine, -sine)
    weight = np.where(harmonic == 0, 1.0, 2.0)[:, None] * retained ** (-0.5)
    return table * weight, table.T * (math.sqrt(retained) / extent)


def plane_tables(extent, retained, groups):
    rows = retained // groups
    places = np.arange(retained)
    wave_y = wave_table(retained)[places % rows * groups + places // rows]
    cosine, sine = trig_table(np.arange(extent), wave_y, extent)
    inverse_y = np.concatenate([cosine, sine], axis=1) * retained ** (-0.5)
    forward_y = np.concatenate([cosine.T, -sine.T], axis=1) * (math.sqrt(retained) / extent)
    inverse_last, forward_last = z_tables(extent, retained)
    halfway = retained // 2
    turn = np.where(places < halfway, -1.0, 1.0)
    wave_z = (places % halfway).astype(np.float32)
    lanes = np.zeros((8, retained), np.float32)
    lanes[0], lanes[1] = turn, wave_z
    column = np.broadcast_to(wave_y[:, None], (retained, retained)).astype(np.float32)
    tables = [lanes, column]
    for table in (inverse_y, inverse_last, forward_last, forward_y):
        tables += split_table(table)
    return [jnp.asarray(t) for t in tables]


def plane_math(fields, tables):
    lanes, wave_y, iy0, iy1, iz0, iz1, fz0, fz1, fy0, fy1 = tables
    turn, wave_z = lanes[0:1, :], lanes[1:2, :]
    retained = wave_y.shape[0]
    extent = iy0.shape[0]

    def turned(values):
        return pltpu.roll(values, retained // 2, 1) * turn

    v0, v1, v2, d1, d2 = fields
    i0 = turned(v0)
    w0 = turned(wave_y * v2 - wave_z * v1)
    w1 = wave_z * i0 - d2
    w2 = d1 - wave_y * i0
    six = (v0, v1, v2, w0, w1, w2)
    stacked = jnp.concatenate(
        [jnp.concatenate(six, axis=1), jnp.concatenate([i0] + [turned(f) for f in six[1:]], axis=1)],
        axis=0,
    )
    along_y = dot3((iy0, iy1), split(stacked))
    rows = jnp.concatenate(
        [along_y[:, f * retained : (f + 1) * retained] for f in range(6)], axis=0
    )
    physical = dot3(split(rows), (iz0, iz1))
    u0, u1, u2, w0, w1, w2 = [physical[f * extent : (f + 1) * extent] for f in range(6)]
    product = jnp.concatenate([u1 * w2 - u2 * w1, u2 * w0 - u0 * w2, u0 * w1 - u1 * w0], axis=0)
    along_z = dot3(split(product), (fz0, fz1))
    parts = [along_z[f * extent : (f + 1) * extent] for f in range(3)]
    stacked = jnp.concatenate(
        [jnp.concatenate(parts, axis=1), jnp.concatenate([turned(p) for p in parts], axis=1)],
        axis=0,
    )
    result = dot3((fy0, fy1), split(stacked))
    return [result[:, f * retained : (f + 1) * retained] for f in range(3)]


def plane_kernel(*refs):
    recv, out = refs[0], refs[-1]
    tables = [ref[...] for ref in refs[1:-1]]
    groups, _, _, rows, retained = recv.shape
    fields = [recv[:, 0, f].reshape(groups * rows, retained) for f in range(5)]
    for f, values in enumerate(plane_math(fields, tables)):
        out[:, 0, f] = values.reshape(groups, rows, retained)


def evaluate_planes(recv, tables):
    groups, planes, _, rows, retained = recv.shape

    def whole(table):
        return pl.BlockSpec(table.shape, lambda i: (0, 0))

    return pl.pallas_call(
        plane_kernel,
        grid=(planes,),
        in_specs=[pl.BlockSpec((groups, 1, 5, rows, retained), lambda i: (0, i, 0, 0, 0))]
        + [whole(t) for t in tables],
        out_specs=pl.BlockSpec((groups, 1, 3, rows, retained), lambda i: (0, i, 0, 0, 0)),
        out_shape=jax.ShapeDtypeStruct((groups, planes, 3, rows, retained), jnp.float32),
        compiler_params=pltpu.CompilerParams(vmem_limit_bytes=50 * 1024 * 1024),
        cost_estimate=pl.CostEstimate(flops=10**10, bytes_accessed=4 * 10**6, transcendentals=0),
        name="planes",
    )(recv, *tables)


def exchange_kernel(gathering, send, recv, send_sems, recv_sems, local_sem):
    halves = lax.axis_size("tm")
    count_py, count_pz = lax.axis_size("py"), lax.axis_size("pz")
    groups = count_py * count_pz
    position = lax.axis_index("tm")
    member = lax.axis_index("py") * count_pz + lax.axis_index("pz")
    own_slot = position * groups + member if gathering else member
    own_part = member if gathering else position * groups + member
    parts = groups if gathering else halves * groups
    slots = halves * groups if gathering else groups

    def copy(part, to_half, to_member, slot):
        return pltpu.make_async_remote_copy(
            src_ref=send.at[part],
            dst_ref=recv.at[slot],
            send_sem=send_sems.at[part],
            recv_sem=recv_sems.at[slot],
            device_id={"tm": to_half, "py": to_member // count_pz, "pz": lax.rem(to_member, count_pz)},
            device_id_type=pl.DeviceIdType.MESH,
        )

    def target(step):
        to_member = lax.rem(member + step, groups)
        if gathering:
            return to_member, halves - 1, to_member
        to_half = lax.rem(step // groups + position + 1, halves)
        return to_half * groups + to_member, to_half, to_member

    local = pltpu.make_async_copy(send.at[own_part], recv.at[own_slot], local_sem)

    def is_self(to_half, to_member):
        return jnp.logical_and(to_half == position, to_member == member)

    def push(step, carry):
        part, to_half, to_member = target(step)

        @pl.when(jnp.logical_not(is_self(to_half, to_member)))
        def _():
            copy(part, to_half, to_member, own_slot).start()

        return carry

    def drain(step, carry):
        part, to_half, to_member = target(step)

        @pl.when(jnp.logical_not(is_self(to_half, to_member)))
        def _():
            copy(part, to_half, to_member, own_slot).wait_send()

        return carry

    def take(slot, carry):
        from_self = jnp.logical_and(
            slot == own_slot, position == (halves - 1 if gathering else 0)
        )

        @pl.when(jnp.logical_not(from_self))
        def _():
            copy(0, position, member, slot).wait_recv()

        return carry

    sends = position >= 0 if gathering else position == 0
    takes = position == halves - 1 if gathering else position >= 0
    keeps = position == (halves - 1 if gathering else 0)

    @pl.when(sends)
    def _():
        lax.fori_loop(0, parts, push, 0)

    @pl.when(keeps)
    def _():
        local.start()

    @pl.when(takes)
    def _():
        lax.fori_loop(0, slots, take, 0)

    @pl.when(sends)
    def _():
        lax.fori_loop(0, parts, drain, 0)

    @pl.when(keeps)
    def _():
        local.wait()


def exchange(send, gathering, groups, halves):
    parts = groups if gathering else halves * groups
    slots = halves * groups if gathering else groups
    return pl.pallas_call(
        partial(exchange_kernel, gathering),
        in_specs=[pl.BlockSpec(memory_space=pl.ANY)],
        out_specs=pl.BlockSpec(memory_space=pl.ANY),
        out_shape=jax.ShapeDtypeStruct((slots,) + send.shape[1:], jnp.float32),
        scratch_shapes=[
            pltpu.SemaphoreType.DMA((parts,)),
            pltpu.SemaphoreType.DMA((slots,)),
            pltpu.SemaphoreType.DMA,
        ],
        compiler_params=pltpu.CompilerParams(has_side_effects=True),
        name="gather" if gathering else "scatter",
    )(send)


def helped_advance(stored, state, wavegrid, groups, halves):
    wave_x, wave_y, wave_z = wavegrid
    retained = stored.shape[-1]
    rows = stored.shape[2]
    extent = 3 * retained // 2
    planes = extent // (groups * halves)
    seeds = jnp.concatenate([state, rotate(wave_x * state[1:3])], axis=0)
    cosine, sine = trig_table(np.arange(extent), wave_table(retained), extent)
    inverse_x = np.concatenate([cosine, sine], axis=1) * retained ** (-0.5)
    both = jnp.concatenate([seeds, rotate(seeds)], axis=1)
    moved = jnp.einsum(
        "xk,fkar->xfar", jnp.asarray(inverse_x, jnp.float32), both, precision=lax.Precision.HIGH
    )
    send = moved.reshape(halves * groups, planes, 5, rows, retained)
    recv = exchange(send, False, groups, halves)
    recv, stored = lax.optimization_barrier((recv, stored))
    earlier = shifted(stored, "tm", 1)
    returned = evaluate_planes(recv, plane_tables(extent, retained, groups))
    arrived = exchange(returned, True, groups, halves).reshape(extent, 3, rows, retained)
    forward_x = np.concatenate([cosine.T, -sine.T], axis=1) * (math.sqrt(retained) / extent)
    both = jnp.concatenate([arrived, rotate(arrived)], axis=0)
    nonlinear = jnp.einsum(
        "kx,xfar->fkar", jnp.asarray(forward_x, jnp.float32), both, precision=lax.Precision.HIGH
    )
    squared = wave_x * wave_x + wave_y * wave_y + wave_z * wave_z
    damping = jnp.exp(-viscosity * time_step * squared)
    return damping * project(earlier + time_step * nonlinear, wavegrid)


def shards(start_states):
    count_py = lax.axis_size("py")
    count_pz = lax.axis_size("pz")
    groups = count_py * count_pz
    member = lax.axis_index("py") * count_pz + lax.axis_index("pz")
    layout = (count_py, count_pz, groups, member)
    position = lax.axis_index("tm")
    slices = lax.axis_size("tm")
    retained = start_states.shape[-1]
    stored = start_states.reshape(3, retained, start_states.shape[3], retained)
    spectral_state = project(stored, wave_grid(retained, layout))
    if slices == 2:
        earlier_end = helped_advance(
            stored, spectral_state, wave_grid(retained, layout), groups, slices
        )
        result = jnp.where(position == 0, spectral_state, earlier_end)
        return result.reshape(1, result.shape[0], retained, result.shape[2], 1, retained)
    fine_end = advance(spectral_state, "fine", layout)
    coarse_start = restrict(spectral_state, M, groups)
    coarse_next = advance(coarse_start, "coarse", layout)
    fine_low = restrict(fine_end, M, groups)
    correction = fine_low - coarse_next

    def relay(chained):
        return shifted(chained, "tm", 1)

    current = jnp.where(position == 1, relay(fine_low), coarse_start)

    def sweep_turn(turn_index, current):
        candidate = advance(current, "coarse", layout) + correction
        arrived = relay(candidate)
        return jnp.where(position == turn_index + 1, arrived, current)

    current = lax.fori_loop(1, slices - 1, sweep_turn, current)
    upper_band = fine_end - prolong(fine_low, retained, groups)
    previous = shifted(upper_band, "tm", 1)
    updated = prolong(current, retained, groups) + previous
    result = jnp.where(position == 0, spectral_state, updated)
    return result.reshape(1, result.shape[0], retained, result.shape[2], 1, retained)


def solution(mesh):
    in_specs = (P("tm", None, None, None, ("py", "pz"), None),)
    out_specs = P("tm", None, None, None, ("py", "pz"), None)
    return jax.shard_map(shards, mesh=mesh, in_specs=in_specs, out_specs=out_specs, check_vma=False)
```

```python
from functools import partial
import math

import jax
import jax.numpy as jnp
from jax import lax
import numpy as np
from jax.experimental import pallas as pl
from jax.experimental.pallas import tpu as pltpu
from jax.sharding import PartitionSpec as P

M = 64


viscosity = 0.03
time_step = 0.004
highest = lax.Precision.HIGHEST


def shifted(block, axis, distance):
    devices = range(lax.axis_size(axis))
    route = [(i - distance, i) for i in devices if i - distance in devices]
    return lax.ppermute(block, axis, route)


def signed_wave(places, length):
    return jnp.where(places < length // 2, places, places - length)


def rotate(values):
    halfway = values.shape[-1] // 2
    return jnp.concatenate([-values[..., halfway:], values[..., :halfway]], axis=-1)


def trig_pair(outer, inner, extent, factor):
    residue = jnp.mod(outer[:, None] * inner[None, :], extent)
    radians = residue.astype(jnp.float32) * (2.0 * math.pi / extent)
    return (jnp.cos(radians) * factor, jnp.sin(radians) * factor)


def complex_apply(cosine_part, sine_part, values, contracted, direction_sign):
    kernel = jnp.stack(
        [
            jnp.stack([cosine_part, -direction_sign * sine_part]),
            jnp.stack([direction_sign * sine_part, cosine_part]),
        ]
    )
    halfway = values.shape[-1] // 2
    split = values.reshape(values.shape[:-1] + (2, halfway))
    if contracted == 1:
        pattern = "pqok,fkaqh->foaph"
    else:
        pattern = "pqok,flkqh->floph"
    result = jnp.einsum(pattern, kernel, split, precision=highest)
    return result.reshape(result.shape[:-2] + (2 * halfway,))


def inverse_z(extent, retained):
    halfway = retained // 2
    columns = jnp.arange(retained, dtype=jnp.int32)
    harmonic = columns % halfway
    weight = jnp.where(harmonic == 0, 1.0, 2.0) * retained ** (-0.5)
    residue = jnp.mod(harmonic[:, None] * jnp.arange(extent, dtype=jnp.int32)[None, :], extent)
    radians = residue.astype(jnp.float32) * (2.0 * math.pi / extent)
    return (
        jnp.where((columns < halfway)[:, None], jnp.cos(radians), -jnp.sin(radians))
        * weight[:, None]
    )


def forward_z(extent, retained):
    halfway = retained // 2
    columns = jnp.arange(retained, dtype=jnp.int32)
    harmonic = columns % halfway
    residue = jnp.mod(jnp.arange(extent, dtype=jnp.int32)[:, None] * harmonic[None, :], extent)
    radians = residue.astype(jnp.float32) * (2.0 * math.pi / extent)
    return jnp.where((columns < halfway)[None, :], jnp.cos(radians), -jnp.sin(radians)) * (
        math.sqrt(retained) / extent
    )


def inverse_tail(portion, extent, sectioned, layout):
    count_py, count_pz, groups, member = layout
    retained = portion.shape[2]
    local_rows = retained // groups
    places = jnp.arange(retained, dtype=jnp.int32)
    owners = places // local_rows
    wave_y = signed_wave(places % local_rows * groups + owners, retained)
    points = jnp.arange(extent, dtype=jnp.int32)
    cosine_part, sine_part = trig_pair(points, wave_y, extent, retained ** (-0.5))
    along_y = complex_apply(cosine_part, sine_part, portion, 2, 1.0)
    return jnp.einsum("flyr,rz->flyz", along_y, inverse_z(extent, retained), precision=highest)


def forward_tail(portion, retained, sectioned, layout):
    count_py, count_pz, groups, member = layout
    extent = portion.shape[1]
    local_rows = extent // groups
    places = jnp.arange(extent, dtype=jnp.int32)
    points = places // local_rows * local_rows + places % local_rows
    wave_x = signed_wave(jnp.arange(retained, dtype=jnp.int32), retained)
    cosine_part, sine_part = trig_pair(wave_x, points, extent, math.sqrt(retained) / extent)
    return complex_apply(cosine_part, sine_part, portion, 1, -1.0)


def to_physical(coeffs, wavegrid, extent, resolution, layout):
    wave_x, wave_y, wave_z = wavegrid
    retained = coeffs.shape[1]
    seeds = jnp.concatenate([coeffs, wave_x * coeffs[1:3]], axis=0)
    points = jnp.arange(extent, dtype=jnp.int32)
    wave_rows = signed_wave(jnp.arange(retained, dtype=jnp.int32), retained)
    cosine_part, sine_part = trig_pair(points, wave_rows, extent, retained ** (-0.5))
    moved_x = complex_apply(cosine_part, sine_part, seeds, 1, 1.0)
    curl_x = rotate(wave_y * moved_x[2] - wave_z * moved_x[1])
    curl_y = rotate(wave_z * moved_x[0] - moved_x[4])
    curl_z = rotate(moved_x[3] - wave_y * moved_x[0])
    spread = jnp.concatenate([moved_x[:3], jnp.stack([curl_x, curl_y, curl_z])], axis=0)
    if resolution == "coarse":
        finish = partial(inverse_tail, extent=extent, sectioned=False, layout=layout)
        return finish(lax.all_to_all(spread, ("py", "pz"), split_axis=1, concat_axis=2, tiled=True))
    else:
        finish = partial(inverse_tail, extent=extent, sectioned=False, layout=layout)
        return finish(lax.all_to_all(spread, ("py", "pz"), split_axis=1, concat_axis=2, tiled=True))


def to_spectral(fields, retained, resolution, layout):
    count_py, count_pz, groups, member = layout
    extent = fields.shape[-1]
    along_z = jnp.einsum("flyz,zr->flyr", fields, forward_z(extent, retained), precision=highest)
    local_rows = retained // groups
    places = jnp.arange(retained, dtype=jnp.int32)
    wave_y = signed_wave(places % local_rows * groups + places // local_rows, retained)
    cosine_part, sine_part = trig_pair(
        wave_y, jnp.arange(extent, dtype=jnp.int32), extent, math.sqrt(retained) / extent
    )
    along_y = complex_apply(cosine_part, sine_part, along_z, 2, -1.0)
    if resolution == "coarse":
        finish = partial(forward_tail, retained=retained, sectioned=False, layout=layout)
        return finish(
            lax.all_to_all(along_y, ("py", "pz"), split_axis=2, concat_axis=1, tiled=True)
        )
    else:
        finish = partial(forward_tail, retained=retained, sectioned=False, layout=layout)
        return finish(
            lax.all_to_all(along_y, ("py", "pz"), split_axis=2, concat_axis=1, tiled=True)
        )


def wave_grid(retained, layout):
    count_py, count_pz, groups, member = layout
    places = jnp.arange(retained, dtype=jnp.int32)
    wave_x = signed_wave(places, retained).astype(jnp.float32)[:, None, None]
    local_places = jnp.arange(retained // groups, dtype=jnp.int32)
    wave_y = signed_wave(local_places * groups + member, retained).astype(jnp.float32)[
        None, :, None
    ]
    wave_z = (places % (retained // 2)).astype(jnp.float32)[None, None, :]
    return (wave_x, wave_y, wave_z)


def project(coeffs, wavegrid):
    wave_x, wave_y, wave_z = wavegrid
    squared = wave_x * wave_x + wave_y * wave_y + wave_z * wave_z
    divergence = (wave_x * coeffs[0] + wave_y * coeffs[1] + wave_z * coeffs[2]) / jnp.maximum(
        squared, 1.0
    )
    return jnp.stack(
        [
            coeffs[0] - wave_x * divergence,
            coeffs[1] - wave_y * divergence,
            coeffs[2] - wave_z * divergence,
        ]
    )


def cross_product(first_field, second_field):
    return jnp.stack(
        [
            first_field[1] * second_field[2] - first_field[2] * second_field[1],
            first_field[2] * second_field[0] - first_field[0] * second_field[2],
            first_field[0] * second_field[1] - first_field[1] * second_field[0],
        ]
    )


def advance(coeffs, resolution, layout):
    retained = coeffs.shape[1]
    extent = 3 * retained // 2
    wavegrid = wave_grid(retained, layout)
    fields = to_physical(coeffs, wavegrid, extent, resolution, layout)
    product = cross_product(fields[:3], fields[3:])
    nonlinear = to_spectral(product, retained, resolution, layout)
    wave_x, wave_y, wave_z = wavegrid
    squared = wave_x * wave_x + wave_y * wave_y + wave_z * wave_z
    damping = jnp.exp(-viscosity * time_step * squared)
    return damping * (coeffs + time_step * project(nonlinear, wavegrid))


def restrict(coeffs, kept, groups):
    halfway = kept // 2
    retained = coeffs.shape[1]
    rows_kept = jnp.concatenate([coeffs[:, :halfway], coeffs[:, retained - halfway :]], axis=1)
    local_rows = coeffs.shape[2]
    local_kept = kept // groups // 2
    rows_kept = jnp.concatenate(
        [rows_kept[:, :, :local_kept], rows_kept[:, :, local_rows - local_kept :]], axis=2
    )
    columns_half = coeffs.shape[3] // 2
    return jnp.concatenate(
        [rows_kept[..., :halfway], rows_kept[..., columns_half : columns_half + halfway]], axis=3
    )


def prolong(coeffs, retained, groups):
    components, kept, local_kept, width = coeffs.shape
    halfway = kept // 2
    zeros_x = jnp.zeros((components, retained - kept, local_kept, width), jnp.float32)
    wider = jnp.concatenate([coeffs[:, :halfway], zeros_x, coeffs[:, halfway:]], axis=1)
    local_rows = retained // groups
    split_rows = local_kept // 2
    zeros_y = jnp.zeros((components, retained, local_rows - local_kept, width), jnp.float32)
    wider = jnp.concatenate([wider[:, :, :split_rows], zeros_y, wider[:, :, split_rows:]], axis=2)
    zeros_z = jnp.zeros((components, retained, local_rows, retained // 2 - halfway), jnp.float32)
    return jnp.concatenate([wider[..., :halfway], zeros_z, wider[..., halfway:], zeros_z], axis=3)


def wave_table(length):
    places = np.arange(length)
    return np.where(places < length // 2, places, places - length)


def trig_table(outer, inner, extent):
    radians = 2.0 * np.pi / extent * np.mod(np.outer(outer, inner), extent)
    return np.cos(radians), np.sin(radians)


def split_table(table):
    table = np.asarray(table, np.float32)
    high = table.astype(jnp.bfloat16)
    low = (table - high.astype(np.float32)).astype(jnp.bfloat16)
    return high, low


def split(values):
    high = values.astype(jnp.bfloat16)
    low = (values - high.astype(jnp.float32)).astype(jnp.bfloat16)
    return high, low


def dot3(left, right):
    def dot(a, b):
        return jnp.dot(a, b, preferred_element_type=jnp.float32)

    return dot(left[0], right[0]) + dot(left[0], right[1]) + dot(left[1], right[0])


def z_tables(extent, retained):
    halfway = retained // 2
    columns = np.arange(retained)
    harmonic = columns % halfway
    cosine, sine = trig_table(harmonic, np.arange(extent), extent)
    table = np.where((columns < halfway)[:, None], cosine, -sine)
    weight = np.where(harmonic == 0, 1.0, 2.0)[:, None] * retained ** (-0.5)
    return table * weight, table.T * (math.sqrt(retained) / extent)


def plane_tables(extent, retained, groups):
    rows = retained // groups
    places = np.arange(retained)
    wave_y = wave_table(retained)[places % rows * groups + places // rows]
    cosine, sine = trig_table(np.arange(extent), wave_y, extent)
    inverse_y = np.concatenate([cosine, sine], axis=1) * retained ** (-0.5)
    forward_y = np.concatenate([cosine.T, -sine.T], axis=1) * (math.sqrt(retained) / extent)
    inverse_last, forward_last = z_tables(extent, retained)
    halfway = retained // 2
    turn = np.where(places < halfway, -1.0, 1.0)
    wave_z = (places % halfway).astype(np.float32)
    lanes = np.zeros((8, retained), np.float32)
    lanes[0], lanes[1] = turn, wave_z
    column = np.broadcast_to(wave_y[:, None], (retained, retained)).astype(np.float32)
    tables = [lanes, column]
    for table in (inverse_y, inverse_last, forward_last, forward_y):
        tables += split_table(table)
    return [jnp.asarray(t) for t in tables]


def plane_math(fields, tables):
    lanes, wave_y, iy0, iy1, iz0, iz1, fz0, fz1, fy0, fy1 = tables
    turn, wave_z = lanes[0:1, :], lanes[1:2, :]
    retained = wave_y.shape[0]
    extent = iy0.shape[0]

    def turned(values):
        return pltpu.roll(values, retained // 2, 1) * turn

    v0, v1, v2, d1, d2 = fields
    i0 = turned(v0)
    w0 = turned(wave_y * v2 - wave_z * v1)
    w1 = wave_z * i0 - d2
    w2 = d1 - wave_y * i0
    six = (v0, v1, v2, w0, w1, w2)
    stacked = jnp.concatenate(
        [jnp.concatenate(six, axis=1), jnp.concatenate([i0] + [turned(f) for f in six[1:]], axis=1)],
        axis=0,
    )
    along_y = dot3((iy0, iy1), split(stacked))
    rows = jnp.concatenate(
        [along_y[:, f * retained : (f + 1) * retained] for f in range(6)], axis=0
    )
    physical = dot3(split(rows), (iz0, iz1))
    u0, u1, u2, w0, w1, w2 = [physical[f * extent : (f + 1) * extent] for f in range(6)]
    product = jnp.concatenate([u1 * w2 - u2 * w1, u2 * w0 - u0 * w2, u0 * w1 - u1 * w0], axis=0)
    along_z = dot3(split(product), (fz0, fz1))
    parts = [along_z[f * extent : (f + 1) * extent] for f in range(3)]
    stacked = jnp.concatenate(
        [jnp.concatenate(parts, axis=1), jnp.concatenate([turned(p) for p in parts], axis=1)],
        axis=0,
    )
    result = dot3((fy0, fy1), split(stacked))
    return [result[:, f * retained : (f + 1) * retained] for f in range(3)]


def x_tables(extent, retained, halves):
    wave_x = wave_table(retained)
    cosine, sine = trig_table(np.arange(extent), wave_x, extent)
    values = np.concatenate([cosine, sine], axis=1)
    slopes = np.concatenate([-sine * wave_x, cosine * wave_x], axis=1)
    per_half = [table.reshape(halves, extent // halves, -1) for table in (values, slopes)]
    table = np.concatenate(per_half, axis=1) * retained ** (-0.5)
    return [jnp.asarray(t) for t in split_table(table)]


def step_kernel(*refs):
    state, x0, x1 = refs[:3]
    table_refs = refs[3:13]
    out, earlier = refs[13:15]
    spread, recv, result = refs[15:18]
    state_send, state_recv, field_send, field_recv, back_send, back_recv = refs[18:]
    _, planes, groups, rows, retained = spread.shape
    count_pz = lax.axis_size("pz")
    position = lax.axis_index("tm")
    row, place = lax.axis_index("py"), lax.axis_index("pz")
    member = row * count_pz + place
    half_points = planes * groups

    def remote(source, target, send_sem, recv_sem, half, to_member):
        return pltpu.make_async_remote_copy(
            src_ref=source,
            dst_ref=target,
            send_sem=send_sem,
            recv_sem=recv_sem,
            device_id={"tm": half, "py": to_member // count_pz, "pz": lax.rem(to_member, count_pz)},
            device_id_type=pl.DeviceIdType.MESH,
        )

    def state_copy(f):
        return remote(state.at[f], earlier.at[f], state_send.at[f], state_recv.at[f], 1, member)

    @pl.when(position == 0)
    def _():
        for f in (1, 2, 0):
            state_copy(f).start()
        earlier[...] = state[...]

    turn = table_refs[0][0:1, :]
    tables_x = (x0[position], x1[position])
    for group, f in enumerate((1, 2, 0)):
        first, count = 2 * group, 2 if f else 1

        @pl.when(position == 1)
        def _():
            state_copy(f).wait_recv()

        parts = [earlier[f, a] for a in range(rows)]
        stacked = jnp.concatenate(
            [
                jnp.concatenate(parts, axis=1),
                jnp.concatenate([pltpu.roll(p, retained // 2, 1) * turn for p in parts], axis=1),
            ],
            axis=0,
        )
        moved = dot3([t[: count * half_points] for t in tables_x], split(stacked))
        for c in range(count):
            flat = spread.at[first + c].reshape(half_points * rows, retained)
            for a in range(rows):
                flat[pl.ds(a, half_points, stride=rows), :] = moved[
                    c * half_points : (c + 1) * half_points, a * retained : (a + 1) * retained
                ]
        recv[first : first + count, :, member] = spread[first : first + count, :, member]

        def push(step, carry, first=first, count=count, group=group):
            to_member = lax.rem(member + step, groups)
            remote(
                spread.at[pl.ds(first, count), :, to_member],
                recv.at[pl.ds(first, count), :, member],
                field_send,
                field_recv.at[group],
                position,
                to_member,
            ).start()
            return carry

        lax.fori_loop(1, groups, push, 0)

    for group in range(3):
        some = recv.at[pl.ds(2 * group, 2 if group < 2 else 1), :, pl.ds(0, groups - 1)]
        remote(some, some, field_send, field_recv.at[group], position, member).wait_recv()

    tables = [ref[...] for ref in table_refs]

    def plane(p, carry):
        v1, d1, v2, d2, v0 = [recv[f, p].reshape(groups * rows, retained) for f in range(5)]
        for f, values in enumerate(plane_math([v0, v1, v2, d1, d2], tables)):
            result[p, :, f] = values.reshape(groups, rows, retained)

        def push(step, carry):
            to_member = lax.rem(member + step, groups)

            @pl.when(jnp.logical_or(position == 0, step > 0))
            def _():
                remote(
                    result.at[p, to_member],
                    out.at[position, p, member],
                    back_send,
                    back_recv,
                    1,
                    to_member,
                ).start()

            return carry

        lax.fori_loop(0, groups, push, 0)

        @pl.when(position == 1)
        def _():
            pltpu.make_async_copy(result.at[p, member], out.at[1, p, member], back_recv).start()

        return carry

    lax.fori_loop(0, planes, plane, 0)

    some = spread.at[:, :, pl.ds(0, groups - 1)]
    remote(some, some, field_send, field_recv.at[0], position, member).wait_send()

    @pl.when(position == 0)
    def _():
        for f in range(3):
            state_copy(f).wait_send()
        remote(result, result, back_send, back_recv, 1, member).wait_send()

    @pl.when(position == 1)
    def _():
        some = result.at[:, pl.ds(0, groups - 1)]
        remote(some, some, back_send, back_recv, 1, member).wait_send()
        remote(out, out, back_send, back_recv, 1, member).wait_recv()


def helped_advance(state, wavegrid, groups, halves):
    wave_x, wave_y, wave_z = wavegrid
    retained = state.shape[-1]
    rows = state.shape[2]
    extent = 3 * retained // 2
    planes = extent // (groups * halves)
    tables = x_tables(extent, retained, halves) + plane_tables(extent, retained, groups)
    vmem = pl.BlockSpec(memory_space=pltpu.VMEM)
    turned_state = jnp.swapaxes(state, 1, 2)
    arrived, earlier = pl.pallas_call(
        step_kernel,
        in_specs=[vmem] * (1 + len(tables)),
        out_specs=[pl.BlockSpec(memory_space=pl.ANY), vmem],
        out_shape=[
            jax.ShapeDtypeStruct((halves, planes, groups, 3, rows, retained), jnp.float32),
            jax.ShapeDtypeStruct(turned_state.shape, jnp.float32),
        ],
        scratch_shapes=[
            pltpu.VMEM((5, planes, groups, rows, retained), jnp.float32),
            pltpu.VMEM((5, planes, groups, rows, retained), jnp.float32),
            pltpu.VMEM((planes, groups, 3, rows, retained), jnp.float32),
            pltpu.SemaphoreType.DMA((3,)),
            pltpu.SemaphoreType.DMA((3,)),
            pltpu.SemaphoreType.DMA,
            pltpu.SemaphoreType.DMA((3,)),
            pltpu.SemaphoreType.DMA,
            pltpu.SemaphoreType.DMA,
        ],
        compiler_params=pltpu.CompilerParams(
            has_side_effects=True, vmem_limit_bytes=56 * 1024 * 1024
        ),
        name="step",
    )(turned_state, *tables)
    earlier = jnp.swapaxes(earlier, 1, 2)
    arrived = arrived.reshape(extent, 3, rows, retained)
    cosine, sine = trig_table(wave_table(retained), np.arange(extent), extent)
    forward_x = np.concatenate([cosine, -sine], axis=1) * (math.sqrt(retained) / extent)
    both = jnp.concatenate([arrived, rotate(arrived)], axis=0)
    nonlinear = jnp.einsum(
        "kx,xfar->fkar", jnp.asarray(forward_x, jnp.float32), both, precision=lax.Precision.HIGH
    )
    squared = wave_x * wave_x + wave_y * wave_y + wave_z * wave_z
    damping = jnp.exp(-viscosity * time_step * squared)
    return damping * project(earlier + time_step * nonlinear, wavegrid)


def shards(start_states):
    count_py = lax.axis_size("py")
    count_pz = lax.axis_size("pz")
    groups = count_py * count_pz
    member = lax.axis_index("py") * count_pz + lax.axis_index("pz")
    layout = (count_py, count_pz, groups, member)
    position = lax.axis_index("tm")
    slices = lax.axis_size("tm")
    retained = start_states.shape[-1]
    stored = start_states.reshape(3, retained, start_states.shape[3], retained)
    spectral_state = project(stored, wave_grid(retained, layout))
    if slices == 2:
        earlier_end = helped_advance(
            spectral_state, wave_grid(retained, layout), groups, slices
        )
        result = jnp.where(position == 0, spectral_state, earlier_end)
        return result.reshape(1, result.shape[0], retained, result.shape[2], 1, retained)
    fine_end = advance(spectral_state, "fine", layout)
    coarse_start = restrict(spectral_state, M, groups)
    coarse_next = advance(coarse_start, "coarse", layout)
    fine_low = restrict(fine_end, M, groups)
    correction = fine_low - coarse_next

    def relay(chained):
        return shifted(chained, "tm", 1)

    current = jnp.where(position == 1, relay(fine_low), coarse_start)

    def sweep_turn(turn_index, current):
        candidate = advance(current, "coarse", layout) + correction
        arrived = relay(candidate)
        return jnp.where(position == turn_index + 1, arrived, current)

    current = lax.fori_loop(1, slices - 1, sweep_turn, current)
    upper_band = fine_end - prolong(fine_low, retained, groups)
    previous = shifted(upper_band, "tm", 1)
    updated = prolong(current, retained, groups) + previous
    result = jnp.where(position == 0, spectral_state, updated)
    return result.reshape(1, result.shape[0], retained, result.shape[2], 1, retained)


def solution(mesh):
    in_specs = (P("tm", None, None, None, ("py", "pz"), None),)
    out_specs = P("tm", None, None, None, ("py", "pz"), None)
    return jax.shard_map(shards, mesh=mesh, in_specs=in_specs, out_specs=out_specs, check_vma=False)
```

```python
from functools import partial
import math

import jax
import jax.numpy as jnp
from jax import lax
import numpy as np
from jax.experimental import pallas as pl
from jax.experimental.pallas import tpu as pltpu
from jax.sharding import PartitionSpec as P

M = 64


viscosity = 0.03
time_step = 0.004
highest = lax.Precision.HIGHEST


def shifted(block, axis, distance):
    devices = range(lax.axis_size(axis))
    route = [(i - distance, i) for i in devices if i - distance in devices]
    return lax.ppermute(block, axis, route)


def signed_wave(places, length):
    return jnp.where(places < length // 2, places, places - length)


def rotate(values):
    halfway = values.shape[-1] // 2
    return jnp.concatenate([-values[..., halfway:], values[..., :halfway]], axis=-1)


def trig_pair(outer, inner, extent, factor):
    residue = jnp.mod(outer[:, None] * inner[None, :], extent)
    radians = residue.astype(jnp.float32) * (2.0 * math.pi / extent)
    return (jnp.cos(radians) * factor, jnp.sin(radians) * factor)


def complex_apply(cosine_part, sine_part, values, contracted, direction_sign):
    kernel = jnp.stack(
        [
            jnp.stack([cosine_part, -direction_sign * sine_part]),
            jnp.stack([direction_sign * sine_part, cosine_part]),
        ]
    )
    halfway = values.shape[-1] // 2
    split = values.reshape(values.shape[:-1] + (2, halfway))
    if contracted == 1:
        pattern = "pqok,fkaqh->foaph"
    else:
        pattern = "pqok,flkqh->floph"
    result = jnp.einsum(pattern, kernel, split, precision=highest)
    return result.reshape(result.shape[:-2] + (2 * halfway,))


def inverse_z(extent, retained):
    halfway = retained // 2
    columns = jnp.arange(retained, dtype=jnp.int32)
    harmonic = columns % halfway
    weight = jnp.where(harmonic == 0, 1.0, 2.0) * retained ** (-0.5)
    residue = jnp.mod(harmonic[:, None] * jnp.arange(extent, dtype=jnp.int32)[None, :], extent)
    radians = residue.astype(jnp.float32) * (2.0 * math.pi / extent)
    return (
        jnp.where((columns < halfway)[:, None], jnp.cos(radians), -jnp.sin(radians))
        * weight[:, None]
    )


def forward_z(extent, retained):
    halfway = retained // 2
    columns = jnp.arange(retained, dtype=jnp.int32)
    harmonic = columns % halfway
    residue = jnp.mod(jnp.arange(extent, dtype=jnp.int32)[:, None] * harmonic[None, :], extent)
    radians = residue.astype(jnp.float32) * (2.0 * math.pi / extent)
    return jnp.where((columns < halfway)[None, :], jnp.cos(radians), -jnp.sin(radians)) * (
        math.sqrt(retained) / extent
    )


def inverse_tail(portion, extent, sectioned, layout):
    count_py, count_pz, groups, member = layout
    retained = portion.shape[2]
    local_rows = retained // groups
    places = jnp.arange(retained, dtype=jnp.int32)
    owners = places // local_rows
    wave_y = signed_wave(places % local_rows * groups + owners, retained)
    points = jnp.arange(extent, dtype=jnp.int32)
    cosine_part, sine_part = trig_pair(points, wave_y, extent, retained ** (-0.5))
    along_y = complex_apply(cosine_part, sine_part, portion, 2, 1.0)
    return jnp.einsum("flyr,rz->flyz", along_y, inverse_z(extent, retained), precision=highest)


def forward_tail(portion, retained, sectioned, layout):
    count_py, count_pz, groups, member = layout
    extent = portion.shape[1]
    local_rows = extent // groups
    places = jnp.arange(extent, dtype=jnp.int32)
    points = places // local_rows * local_rows + places % local_rows
    wave_x = signed_wave(jnp.arange(retained, dtype=jnp.int32), retained)
    cosine_part, sine_part = trig_pair(wave_x, points, extent, math.sqrt(retained) / extent)
    return complex_apply(cosine_part, sine_part, portion, 1, -1.0)


def to_physical(coeffs, wavegrid, extent, resolution, layout):
    wave_x, wave_y, wave_z = wavegrid
    retained = coeffs.shape[1]
    seeds = jnp.concatenate([coeffs, wave_x * coeffs[1:3]], axis=0)
    points = jnp.arange(extent, dtype=jnp.int32)
    wave_rows = signed_wave(jnp.arange(retained, dtype=jnp.int32), retained)
    cosine_part, sine_part = trig_pair(points, wave_rows, extent, retained ** (-0.5))
    moved_x = complex_apply(cosine_part, sine_part, seeds, 1, 1.0)
    curl_x = rotate(wave_y * moved_x[2] - wave_z * moved_x[1])
    curl_y = rotate(wave_z * moved_x[0] - moved_x[4])
    curl_z = rotate(moved_x[3] - wave_y * moved_x[0])
    spread = jnp.concatenate([moved_x[:3], jnp.stack([curl_x, curl_y, curl_z])], axis=0)
    if resolution == "coarse":
        finish = partial(inverse_tail, extent=extent, sectioned=False, layout=layout)
        return finish(lax.all_to_all(spread, ("py", "pz"), split_axis=1, concat_axis=2, tiled=True))
    else:
        finish = partial(inverse_tail, extent=extent, sectioned=False, layout=layout)
        return finish(lax.all_to_all(spread, ("py", "pz"), split_axis=1, concat_axis=2, tiled=True))


def to_spectral(fields, retained, resolution, layout):
    count_py, count_pz, groups, member = layout
    extent = fields.shape[-1]
    along_z = jnp.einsum("flyz,zr->flyr", fields, forward_z(extent, retained), precision=highest)
    local_rows = retained // groups
    places = jnp.arange(retained, dtype=jnp.int32)
    wave_y = signed_wave(places % local_rows * groups + places // local_rows, retained)
    cosine_part, sine_part = trig_pair(
        wave_y, jnp.arange(extent, dtype=jnp.int32), extent, math.sqrt(retained) / extent
    )
    along_y = complex_apply(cosine_part, sine_part, along_z, 2, -1.0)
    if resolution == "coarse":
        finish = partial(forward_tail, retained=retained, sectioned=False, layout=layout)
        return finish(
            lax.all_to_all(along_y, ("py", "pz"), split_axis=2, concat_axis=1, tiled=True)
        )
    else:
        finish = partial(forward_tail, retained=retained, sectioned=False, layout=layout)
        return finish(
            lax.all_to_all(along_y, ("py", "pz"), split_axis=2, concat_axis=1, tiled=True)
        )


def wave_grid(retained, layout):
    count_py, count_pz, groups, member = layout
    places = jnp.arange(retained, dtype=jnp.int32)
    wave_x = signed_wave(places, retained).astype(jnp.float32)[:, None, None]
    local_places = jnp.arange(retained // groups, dtype=jnp.int32)
    wave_y = signed_wave(local_places * groups + member, retained).astype(jnp.float32)[
        None, :, None
    ]
    wave_z = (places % (retained // 2)).astype(jnp.float32)[None, None, :]
    return (wave_x, wave_y, wave_z)


def project(coeffs, wavegrid):
    wave_x, wave_y, wave_z = wavegrid
    squared = wave_x * wave_x + wave_y * wave_y + wave_z * wave_z
    divergence = (wave_x * coeffs[0] + wave_y * coeffs[1] + wave_z * coeffs[2]) / jnp.maximum(
        squared, 1.0
    )
    return jnp.stack(
        [
            coeffs[0] - wave_x * divergence,
            coeffs[1] - wave_y * divergence,
            coeffs[2] - wave_z * divergence,
        ]
    )


def cross_product(first_field, second_field):
    return jnp.stack(
        [
            first_field[1] * second_field[2] - first_field[2] * second_field[1],
            first_field[2] * second_field[0] - first_field[0] * second_field[2],
            first_field[0] * second_field[1] - first_field[1] * second_field[0],
        ]
    )


def advance(coeffs, resolution, layout):
    retained = coeffs.shape[1]
    extent = 3 * retained // 2
    wavegrid = wave_grid(retained, layout)
    fields = to_physical(coeffs, wavegrid, extent, resolution, layout)
    product = cross_product(fields[:3], fields[3:])
    nonlinear = to_spectral(product, retained, resolution, layout)
    wave_x, wave_y, wave_z = wavegrid
    squared = wave_x * wave_x + wave_y * wave_y + wave_z * wave_z
    damping = jnp.exp(-viscosity * time_step * squared)
    return damping * (coeffs + time_step * project(nonlinear, wavegrid))


def restrict(coeffs, kept, groups):
    halfway = kept // 2
    retained = coeffs.shape[1]
    rows_kept = jnp.concatenate([coeffs[:, :halfway], coeffs[:, retained - halfway :]], axis=1)
    local_rows = coeffs.shape[2]
    local_kept = kept // groups // 2
    rows_kept = jnp.concatenate(
        [rows_kept[:, :, :local_kept], rows_kept[:, :, local_rows - local_kept :]], axis=2
    )
    columns_half = coeffs.shape[3] // 2
    return jnp.concatenate(
        [rows_kept[..., :halfway], rows_kept[..., columns_half : columns_half + halfway]], axis=3
    )


def prolong(coeffs, retained, groups):
    components, kept, local_kept, width = coeffs.shape
    halfway = kept // 2
    zeros_x = jnp.zeros((components, retained - kept, local_kept, width), jnp.float32)
    wider = jnp.concatenate([coeffs[:, :halfway], zeros_x, coeffs[:, halfway:]], axis=1)
    local_rows = retained // groups
    split_rows = local_kept // 2
    zeros_y = jnp.zeros((components, retained, local_rows - local_kept, width), jnp.float32)
    wider = jnp.concatenate([wider[:, :, :split_rows], zeros_y, wider[:, :, split_rows:]], axis=2)
    zeros_z = jnp.zeros((components, retained, local_rows, retained // 2 - halfway), jnp.float32)
    return jnp.concatenate([wider[..., :halfway], zeros_z, wider[..., halfway:], zeros_z], axis=3)


def wave_table(length):
    places = np.arange(length)
    return np.where(places < length // 2, places, places - length)


def trig_table(outer, inner, extent):
    radians = 2.0 * np.pi / extent * np.mod(np.outer(outer, inner), extent)
    return np.cos(radians), np.sin(radians)


def split_table(table):
    table = np.asarray(table, np.float32)
    high = table.astype(jnp.bfloat16)
    low = (table - high.astype(np.float32)).astype(jnp.bfloat16)
    return high, low


def split(values):
    high = values.astype(jnp.bfloat16)
    low = (values - high.astype(jnp.float32)).astype(jnp.bfloat16)
    return high, low


def dot3(left, right):
    def dot(a, b):
        return jnp.dot(a, b, preferred_element_type=jnp.float32)

    return dot(left[0], right[0]) + dot(left[0], right[1]) + dot(left[1], right[0])


def z_tables(extent, retained):
    halfway = retained // 2
    columns = np.arange(retained)
    harmonic = columns % halfway
    cosine, sine = trig_table(harmonic, np.arange(extent), extent)
    table = np.where((columns < halfway)[:, None], cosine, -sine)
    weight = np.where(harmonic == 0, 1.0, 2.0)[:, None] * retained ** (-0.5)
    return table * weight, table.T * (math.sqrt(retained) / extent)


def plane_tables(extent, retained, groups):
    rows = retained // groups
    places = np.arange(retained)
    wave_y = wave_table(retained)[places % rows * groups + places // rows]
    cosine, sine = trig_table(np.arange(extent), wave_y, extent)
    inverse_y = np.concatenate([cosine, sine], axis=1) * retained ** (-0.5)
    forward_y = np.concatenate([cosine.T, -sine.T], axis=1) * (math.sqrt(retained) / extent)
    inverse_last, forward_last = z_tables(extent, retained)
    halfway = retained // 2
    turn = np.where(places < halfway, -1.0, 1.0)
    wave_z = (places % halfway).astype(np.float32)
    lanes = np.zeros((8, retained), np.float32)
    lanes[0], lanes[1] = turn, wave_z
    column = np.broadcast_to(wave_y[:, None], (retained, retained)).astype(np.float32)
    tables = [lanes, column]
    for table in (inverse_y, inverse_last, forward_last, forward_y):
        tables += split_table(table)
    return [jnp.asarray(t) for t in tables]


def plane_math(fields, tables):
    lanes, wave_y, iy0, iy1, iz0, iz1, fz0, fz1, fy0, fy1 = tables
    turn, wave_z = lanes[0:1, :], lanes[1:2, :]
    retained = wave_y.shape[0]
    extent = iy0.shape[0]

    def turned(values):
        return pltpu.roll(values, retained // 2, 1) * turn

    v0, v1, v2, d1, d2 = fields
    i0 = turned(v0)
    w0 = turned(wave_y * v2 - wave_z * v1)
    w1 = wave_z * i0 - d2
    w2 = d1 - wave_y * i0
    six = (v0, v1, v2, w0, w1, w2)
    stacked = jnp.concatenate(
        [jnp.concatenate(six, axis=1), jnp.concatenate([i0] + [turned(f) for f in six[1:]], axis=1)],
        axis=0,
    )
    along_y = dot3((iy0, iy1), split(stacked))
    rows = jnp.concatenate(
        [along_y[:, f * retained : (f + 1) * retained] for f in range(6)], axis=0
    )
    physical = dot3(split(rows), (iz0, iz1))
    u0, u1, u2, w0, w1, w2 = [physical[f * extent : (f + 1) * extent] for f in range(6)]
    product = jnp.concatenate([u1 * w2 - u2 * w1, u2 * w0 - u0 * w2, u0 * w1 - u1 * w0], axis=0)
    along_z = dot3(split(product), (fz0, fz1))
    parts = [along_z[f * extent : (f + 1) * extent] for f in range(3)]
    stacked = jnp.concatenate(
        [jnp.concatenate(parts, axis=1), jnp.concatenate([turned(p) for p in parts], axis=1)],
        axis=0,
    )
    result = dot3((fy0, fy1), split(stacked))
    return [result[:, f * retained : (f + 1) * retained] for f in range(3)]


def x_tables(extent, retained, halves):
    wave_x = wave_table(retained)
    cosine, sine = trig_table(np.arange(extent), wave_x, extent)
    values = np.concatenate([cosine, sine], axis=1)
    slopes = np.concatenate([-sine * wave_x, cosine * wave_x], axis=1)
    per_half = [table.reshape(halves, extent // halves, -1) for table in (values, slopes)]
    table = np.concatenate(per_half, axis=1) * retained ** (-0.5)
    return [jnp.asarray(t) for t in split_table(table)]


def step_kernel(*refs):
    state, x0, x1 = refs[:3]
    table_refs = refs[3:13]
    out, earlier = refs[13:15]
    spread, recv, result = refs[15:18]
    state_send, state_recv, field_send, field_recv, back_send, back_recv = refs[18:]
    _, planes, groups, rows, retained = spread.shape
    count_pz = lax.axis_size("pz")
    position = lax.axis_index("tm")
    row, place = lax.axis_index("py"), lax.axis_index("pz")
    member = row * count_pz + place
    half_points = planes * groups

    def remote(source, target, send_sem, recv_sem, half, to_member):
        return pltpu.make_async_remote_copy(
            src_ref=source,
            dst_ref=target,
            send_sem=send_sem,
            recv_sem=recv_sem,
            device_id={"tm": half, "py": to_member // count_pz, "pz": lax.rem(to_member, count_pz)},
            device_id_type=pl.DeviceIdType.MESH,
        )

    count_py = lax.axis_size("py")
    early = planes // 2

    def far_first(step):
        to_place = lax.rem(place + count_pz // 2 + step // count_py, count_pz)
        return lax.rem(row + lax.rem(step, count_py), count_py) * count_pz + to_place

    def state_copy(f):
        return remote(state.at[f], earlier.at[f], state_send.at[f], state_recv.at[f], 1, member)

    @pl.when(position == 0)
    def _():
        for f in (1, 2, 0):
            state_copy(f).start()
        earlier[...] = state[...]

    turn = table_refs[0][0:1, :]
    tables_x = (x0[position], x1[position])
    for group, f in enumerate((1, 2, 0)):
        first, count = 2 * group, 2 if f else 1

        @pl.when(position == 1)
        def _():
            state_copy(f).wait_recv()

        parts = [earlier[f, a] for a in range(rows)]
        stacked = jnp.concatenate(
            [
                jnp.concatenate(parts, axis=1),
                jnp.concatenate([pltpu.roll(p, retained // 2, 1) * turn for p in parts], axis=1),
            ],
            axis=0,
        )
        moved = dot3([t[: count * half_points] for t in tables_x], split(stacked))
        for c in range(count):
            flat = spread.at[first + c].reshape(half_points * rows, retained)
            for a in range(rows):
                flat[pl.ds(a, half_points, stride=rows), :] = moved[
                    c * half_points : (c + 1) * half_points, a * retained : (a + 1) * retained
                ]
        recv[first : first + count, :, member] = spread[first : first + count, :, member]

        batches = [(group, 0, planes)] if f else [(group, 0, early), (group + 1, early, planes)]
        for batch, start, stop in batches:

            def push(step, carry, first=first, count=count, batch=batch, start=start, stop=stop):
                to_member = far_first(step)
                fields, span = pl.ds(first, count), pl.ds(start, stop - start)

                @pl.when(to_member != member)
                def _():
                    remote(
                        spread.at[fields, span, to_member],
                        recv.at[fields, span, member],
                        field_send,
                        field_recv.at[batch],
                        position,
                        to_member,
                    ).start()

                return carry

            lax.fori_loop(0, groups, push, 0)

    def await_fields(batch, first, count, start, stop):
        some = recv.at[pl.ds(first, count), pl.ds(start, stop - start), pl.ds(0, groups - 1)]
        remote(some, some, field_send, field_recv.at[batch], position, member).wait_recv()

    await_fields(0, 0, 2, 0, planes)
    await_fields(1, 2, 2, 0, planes)
    await_fields(2, 4, 1, 0, early)

    tables = [ref[...] for ref in table_refs]

    def plane(p, carry):
        @pl.when(p == early)
        def _():
            await_fields(3, 4, 1, early, planes)

        v1, d1, v2, d2, v0 = [recv[f, p].reshape(groups * rows, retained) for f in range(5)]
        for f, values in enumerate(plane_math([v0, v1, v2, d1, d2], tables)):
            result[p, :, f] = values.reshape(groups, rows, retained)

        def push(step, carry):
            to_member = far_first(step)

            @pl.when(jnp.logical_or(position == 0, to_member != member))
            def _():
                remote(
                    result.at[p, to_member],
                    out.at[position, p, member],
                    back_send,
                    back_recv,
                    1,
                    to_member,
                ).start()

            return carry

        lax.fori_loop(0, groups, push, 0)

        @pl.when(position == 1)
        def _():
            pltpu.make_async_copy(result.at[p, member], out.at[1, p, member], back_recv).start()

        return carry

    lax.fori_loop(0, planes, plane, 0)

    some = spread.at[:, :, pl.ds(0, groups - 1)]
    remote(some, some, field_send, field_recv.at[0], position, member).wait_send()

    @pl.when(position == 0)
    def _():
        for f in range(3):
            state_copy(f).wait_send()
        remote(result, result, back_send, back_recv, 1, member).wait_send()

    @pl.when(position == 1)
    def _():
        some = result.at[:, pl.ds(0, groups - 1)]
        remote(some, some, back_send, back_recv, 1, member).wait_send()
        remote(out, out, back_send, back_recv, 1, member).wait_recv()


def helped_advance(state, wavegrid, groups, halves):
    wave_x, wave_y, wave_z = wavegrid
    retained = state.shape[-1]
    rows = state.shape[2]
    extent = 3 * retained // 2
    planes = extent // (groups * halves)
    tables = x_tables(extent, retained, halves) + plane_tables(extent, retained, groups)
    vmem = pl.BlockSpec(memory_space=pltpu.VMEM)
    turned_state = jnp.swapaxes(state, 1, 2)
    arrived, earlier = pl.pallas_call(
        step_kernel,
        in_specs=[vmem] * (1 + len(tables)),
        out_specs=[pl.BlockSpec(memory_space=pl.ANY), vmem],
        out_shape=[
            jax.ShapeDtypeStruct((halves, planes, groups, 3, rows, retained), jnp.float32),
            jax.ShapeDtypeStruct(turned_state.shape, jnp.float32),
        ],
        scratch_shapes=[
            pltpu.VMEM((5, planes, groups, rows, retained), jnp.float32),
            pltpu.VMEM((5, planes, groups, rows, retained), jnp.float32),
            pltpu.VMEM((planes, groups, 3, rows, retained), jnp.float32),
            pltpu.SemaphoreType.DMA((3,)),
            pltpu.SemaphoreType.DMA((3,)),
            pltpu.SemaphoreType.DMA,
            pltpu.SemaphoreType.DMA((4,)),
            pltpu.SemaphoreType.DMA,
            pltpu.SemaphoreType.DMA,
        ],
        compiler_params=pltpu.CompilerParams(
            has_side_effects=True, vmem_limit_bytes=56 * 1024 * 1024
        ),
        name="step",
    )(turned_state, *tables)
    earlier = jnp.swapaxes(earlier, 1, 2)
    arrived = arrived.reshape(extent, 3, rows, retained)
    cosine, sine = trig_table(wave_table(retained), np.arange(extent), extent)
    forward_x = np.concatenate([cosine, -sine], axis=1) * (math.sqrt(retained) / extent)
    both = jnp.concatenate([arrived, rotate(arrived)], axis=0)
    nonlinear = jnp.einsum(
        "kx,xfar->fkar", jnp.asarray(forward_x, jnp.float32), both, precision=lax.Precision.HIGH
    )
    squared = wave_x * wave_x + wave_y * wave_y + wave_z * wave_z
    damping = jnp.exp(-viscosity * time_step * squared)
    return damping * project(earlier + time_step * nonlinear, wavegrid)


def shards(start_states):
    count_py = lax.axis_size("py")
    count_pz = lax.axis_size("pz")
    groups = count_py * count_pz
    member = lax.axis_index("py") * count_pz + lax.axis_index("pz")
    layout = (count_py, count_pz, groups, member)
    position = lax.axis_index("tm")
    slices = lax.axis_size("tm")
    retained = start_states.shape[-1]
    stored = start_states.reshape(3, retained, start_states.shape[3], retained)
    spectral_state = project(stored, wave_grid(retained, layout))
    if slices == 2:
        earlier_end = helped_advance(
            spectral_state, wave_grid(retained, layout), groups, slices
        )
        result = jnp.where(position == 0, spectral_state, earlier_end)
        return result.reshape(1, result.shape[0], retained, result.shape[2], 1, retained)
    fine_end = advance(spectral_state, "fine", layout)
    coarse_start = restrict(spectral_state, M, groups)
    coarse_next = advance(coarse_start, "coarse", layout)
    fine_low = restrict(fine_end, M, groups)
    correction = fine_low - coarse_next

    def relay(chained):
        return shifted(chained, "tm", 1)

    current = jnp.where(position == 1, relay(fine_low), coarse_start)

    def sweep_turn(turn_index, current):
        candidate = advance(current, "coarse", layout) + correction
        arrived = relay(candidate)
        return jnp.where(position == turn_index + 1, arrived, current)

    current = lax.fori_loop(1, slices - 1, sweep_turn, current)
    upper_band = fine_end - prolong(fine_low, retained, groups)
    previous = shifted(upper_band, "tm", 1)
    updated = prolong(current, retained, groups) + previous
    result = jnp.where(position == 0, spectral_state, updated)
    return result.reshape(1, result.shape[0], retained, result.shape[2], 1, retained)


def solution(mesh):
    in_specs = (P("tm", None, None, None, ("py", "pz"), None),)
    out_specs = P("tm", None, None, None, ("py", "pz"), None)
    return jax.shard_map(shards, mesh=mesh, in_specs=in_specs, out_specs=out_specs, check_vma=False)
```
